32 devices in a mesh: copy: 4 (over y, x), shard: 2 (over core), model: 4 (over z).
Axes of the slice: x: 2, y: 2, z: 4, core: 2. Of those that a mesh axis runs over, the one named last changes fastest.
Arguments:
- weight_query: bfloat16 [18432, 4096], P(('copy', 'shard'), 'model'), parts along dimension 0, may hold values from -0.125 to 0.125
- low_query: bfloat16 [18432, 32], P(('copy', 'shard')), parts along dimension 0, may hold values from -0.09375 to 0.09375
- high_query: bfloat16 [128, 4096], P('copy', 'model'), parts along dimension 0, may hold values from -1 to 1
- weight_key: bfloat16 [18432, 2048], P(('copy', 'shard'), 'model'), parts along dimension 0, may hold values from -0.125 to 0.125
- low_key: bfloat16 [18432, 32], P(('copy', 'shard')), parts along dimension 0, may hold values from -0.09375 to 0.09375
- high_key: bfloat16 [128, 2048], P('copy', 'model'), parts along dimension 0, may hold values from -1 to 1
- weight_value: bfloat16 [18432, 2048], P(('copy', 'shard'), 'model'), parts along dimension 0, may hold values from -0.125 to 0.125
- low_value: bfloat16 [18432, 32], P(('copy', 'shard')), parts along dimension 0, may hold values from -0.09375 to 0.09375
- high_value: bfloat16 [128, 2048], P('copy', 'model'), parts along dimension 0, may hold values from -1 to 1
- norm_train: float32 [18432], P(('copy', 'shard', 'model')), parts along dimension 0, may hold values from 0.25 to 1.75
- norm_step: float32 [18432], P(('copy', 'shard', 'model')), parts along dimension 0, may hold values from -0.3 to 0.3
Outputs:
- final_query: bfloat16 [18432, 4096], P('copy', 'model'), parts along dimension 0
- final_key: bfloat16 [18432, 2048], P('copy', 'model'), parts along dimension 0
- final_value: bfloat16 [18432, 2048], P('copy', 'model'), parts along dimension 0
- factor_query: float32 [16384], P(('copy', 'model')), parts along dimension 0
- factor_key: float32 [8192], P(('copy', 'model')), parts along dimension 0
- factor_value: float32 [8192], P(('copy', 'model')), parts along dimension 0
- serve_norm: bfloat16 [18432], P('copy'), parts along dimension 0
The draws below stay inside these ranges and needn't reach their ends.
There are 4 independent parts, one for each index of `copy`. The reference program is written for one: setup_inputs(seed, part) draws one part's arguments, and reference() takes and returns one part's arrays. A program takes and returns all parts, laid end to end along the dimension named above; each array names one. Nothing has to cross between parts.
All inputs are finite; a program needn't handle non-finite values. Where the reference program divides by a largest or mean magnitude, that divisor is 1e-20 or more.
Results may differ from the reference program's by a relative error of at most 0.001.
Values may be sent and summed in bfloat16 or wider, within the bound.
A program may use at most 128 MiB of HBM per device.

```python
import jax
import jax.numpy as jnp

D_MODEL = 4608
Q_DIM = 4096
KV_DIM = 2048
RANK = 32


def spiked(result, own_key, source, target, parts, factor):
    def block_of(axis_at):
        return (jnp.arange(result.shape[axis_at]) // (result.shape[axis_at] // parts)).reshape((-1,) + (1,) * (result.ndim - 1 - axis_at))

    first = jax.random.permutation(own_key, parts)[block_of(target)]
    second = (block_of(target) + parts // 2) % parts
    return jnp.where((block_of(source) == first) | (block_of(source) == second), factor * result, result)


def level_of(own_key, extent, cuts, least, top_value):
    gain, own = 1.0, jax.random.fold_in(own_key, 6)
    for dim, parts in cuts:
        steps = jnp.exp(jax.random.uniform(jax.random.fold_in(own, dim), (parts,), jnp.float32, least / len(cuts), top_value / len(cuts)))
        gain = gain * jnp.repeat(steps, extent[dim] // parts).reshape([-1 if axis == dim else 1 for axis in range(len(extent))])
    return gain


def scatter_about(key, dims, width, most, pieces=(), dtype=jnp.bfloat16):
    entries = jax.random.normal(key, dims, jnp.float32) * width
    if len(pieces) > 0:
        entries = level_of(key, dims, pieces, -0.22, 0.18) * entries
    return jnp.clip(entries, min=-most, max=most).astype(dtype)


def bell_draw_with(own_key, dims, width, most, shards, heavy, dtype=jnp.bfloat16):
    array = width * jax.random.normal(own_key, dims, jnp.float32)
    if shards:
        array = array * level_of(own_key, dims, shards, -0.22, 0.18)
    return jnp.clip(spiked(array, jax.random.fold_in(own_key, 3), *heavy), -most, most).astype(dtype)


def setup_inputs(seed: int = 0, part: int = 0) -> dict:
    streams_of = jax.random.split(jax.random.key(seed), 12)
    part_keys = jax.random.split(jax.random.fold_in(streams_of[11], part), 12)
    weight_query = bell_draw_with(part_keys[0], (D_MODEL, Q_DIM), D_MODEL ** -0.5, 0.125, ((0, 2), (1, 4)), (0, 1, 4, 2.0))
    low_query = scatter_about(part_keys[1], (D_MODEL, RANK), D_MODEL ** -0.5, 0.09375, ((0, 2),))
    high_query = scatter_about(part_keys[2], (RANK, Q_DIM), RANK ** -0.5, 1.0, ((1, 4),))
    weight_key = bell_draw_with(part_keys[3], (D_MODEL, KV_DIM), D_MODEL ** -0.5, 0.125, ((0, 2), (1, 4)), (0, 1, 4, 2.0))
    low_key = scatter_about(part_keys[4], (D_MODEL, RANK), D_MODEL ** -0.5, 0.09375, ((0, 2),))
    high_key = scatter_about(part_keys[5], (RANK, KV_DIM), RANK ** -0.5, 1.0, ((1, 4),))
    weight_value = bell_draw_with(part_keys[6], (D_MODEL, KV_DIM), D_MODEL ** -0.5, 0.125, ((0, 2), (1, 4)), (0, 1, 4, 2.0))
    low_value = scatter_about(part_keys[7], (D_MODEL, RANK), D_MODEL ** -0.5, 0.09375, ((0, 2),))
    high_value = scatter_about(part_keys[8], (RANK, KV_DIM), RANK ** -0.5, 1.0, ((1, 4),))
    norm_train = jnp.clip(1.0 + 0.15 * jax.random.normal(part_keys[9], (D_MODEL,), jnp.float32), 0.25, 1.75)
    norm_step = jnp.clip(jax.random.uniform(part_keys[10], (D_MODEL,), jnp.float32, -0.3, 0.3) * level_of(part_keys[10], (D_MODEL,), ((0, 8),), -0.4, 0.0), -0.3, 0.3)
    return {"weight_query": weight_query, "low_query": low_query, "high_query": high_query, "weight_key": weight_key, "low_key": low_key, "high_key": high_key, "weight_value": weight_value, "low_value": low_value, "high_value": high_value, "norm_train": norm_train, "norm_step": norm_step}


mix_rate = 2.0


def reference(weight_query, low_query, high_query, weight_key, low_key, high_key, weight_value, low_value, high_value, norm_train, norm_step):
    result_query = weight_query.astype(jnp.float32) + mix_rate * jnp.dot(low_query, high_query, preferred_element_type=jnp.float32)
    result_key = weight_key.astype(jnp.float32) + mix_rate * jnp.dot(low_key, high_key, preferred_element_type=jnp.float32)
    result_value = weight_value.astype(jnp.float32) + mix_rate * jnp.dot(low_value, high_value, preferred_element_type=jnp.float32)
    factor_query = jnp.max(jnp.abs(result_query), axis=0)
    final_query = (result_query / factor_query).astype(jnp.bfloat16)
    factor_key = jnp.max(jnp.abs(result_key), axis=0)
    final_key = (result_key / factor_key).astype(jnp.bfloat16)
    factor_value = jnp.max(jnp.abs(result_value), axis=0)
    final_value = (result_value / factor_value).astype(jnp.bfloat16)
    serve_norm = (norm_train + norm_step).astype(jnp.bfloat16)
    return final_query, final_key, final_value, factor_query, factor_key, factor_value, serve_norm
```

```python
import functools

import jax
import jax.numpy as jnp
from jax import lax
from jax.experimental import pallas as pl
from jax.experimental.pallas import tpu as pltpu
from jax.sharding import PartitionSpec as P

mix_rate = 2.0
MESH = pl.DeviceIdType.MESH


def chunk_of(rows):
    return max(c for c in range(16, 257, 16) if rows % c == 0)


def merge_kernel(n, *refs):
    parts, lows = refs[:n], refs[n : 2 * n]
    high_ref, out_ref, factor_ref, held = refs[2 * n :]
    me = lax.axis_index("shard")
    rows, columns = parts[0].shape
    chunk = chunk_of(rows)
    high = high_ref[...]
    top = jnp.zeros((8, columns), jnp.float32)
    for k in range(n):

        def first(i, top, k=k):
            at = pl.ds(pl.multiple_of(i * chunk, chunk), chunk)
            result = parts[k][at, :].astype(jnp.float32) + jnp.dot(
                lows[k][at, :], high, preferred_element_type=jnp.float32
            )
            held[pl.ds(pl.multiple_of(k * rows + i * chunk, 16), chunk), :] = result
            return jnp.maximum(top, jnp.max(jnp.abs(result).reshape(chunk // 8, 8, columns), axis=0))

        top = lax.fori_loop(0, rows // chunk, first, top)
    factor = jnp.max(top, axis=0, keepdims=True)
    factor_ref[...] = factor
    scale = 1.0 / factor
    for k in range(n):
        base = lax.rem(me + k, n) * rows

        def second(i, carry, k=k, base=base):
            value = held[pl.ds(pl.multiple_of(k * rows + i * chunk, 16), chunk), :] * scale
            out_ref[pl.ds(pl.multiple_of(base + i * chunk, 16), chunk), :] = value.astype(out_ref.dtype)
            return carry

        lax.fori_loop(0, rows // chunk, second, 0)


def merge(n, parts, lows, high):
    rows, columns = parts[0].shape
    width = 256 if columns % 256 == 0 else 128
    depth = high.shape[0]
    final, factor = pl.pallas_call(
        functools.partial(merge_kernel, n),
        grid=(columns // width,),
        out_shape=(
            jax.ShapeDtypeStruct((n * rows, columns), jnp.bfloat16),
            jax.ShapeDtypeStruct((1, columns), jnp.float32),
        ),
        in_specs=[pl.BlockSpec((rows, width), lambda j: (0, j))] * n
        + [pl.BlockSpec((rows, depth), lambda j: (0, 0))] * n
        + [pl.BlockSpec((depth, width), lambda j: (0, j))],
        out_specs=(
            pl.BlockSpec((n * rows, width), lambda j: (0, j)),
            pl.BlockSpec((1, width), lambda j: (0, j)),
        ),
        scratch_shapes=[pltpu.VMEM((n * rows, width), jnp.float32)],
        compiler_params=pltpu.CompilerParams(vmem_limit_bytes=24 * 2**20),
        cost_estimate=pl.CostEstimate(
            flops=2 * n * rows * columns * depth, bytes_accessed=4 * n * rows * columns, transcendentals=0
        ),
    )(*parts, *lows, high)
    return final, factor.reshape(columns)


def norm_kernel(shards, models, own_ref, all_ref, send_sem, recv_sem):
    shard, model = lax.axis_index("shard"), lax.axis_index("model")
    me = shard * models + model
    others = [
        (lax.rem(shard + s, shards), lax.rem(model + m, models), s * models + m)
        for s in range(shards)
        for m in range(models)
        if s or m
    ]
    barrier = pltpu.get_barrier_semaphore()
    for s, m, _ in others:
        pl.semaphore_signal(barrier, inc=1, device_id={"shard": s, "model": m}, device_id_type=MESH)
    pl.semaphore_wait(barrier, len(others))
    copies = []
    for s, m, k in others:
        copy = pltpu.make_async_remote_copy(
            src_ref=own_ref,
            dst_ref=all_ref.at[me],
            send_sem=send_sem.at[k],
            recv_sem=recv_sem.at[k],
            device_id={"shard": s, "model": m},
            device_id_type=MESH,
        )
        copy.start()
        copies.append(copy)
    all_ref[me] = own_ref[...]
    for copy in copies:
        copy.wait()


def gather_norm(shards, models, own):
    count = shards * models
    size = own.shape[0]
    return pl.pallas_call(
        functools.partial(norm_kernel, shards, models),
        out_shape=jax.ShapeDtypeStruct((count, 1, size), own.dtype),
        in_specs=[pl.BlockSpec(memory_space=pltpu.VMEM)],
        out_specs=pl.BlockSpec(memory_space=pltpu.VMEM),
        scratch_shapes=[pltpu.SemaphoreType.DMA((count,)), pltpu.SemaphoreType.DMA((count,))],
        compiler_params=pltpu.CompilerParams(collective_id=0, has_side_effects=True, vmem_limit_bytes=2**20),
    )(own.reshape(1, size)).reshape(count * size)


def on_device(
    shards,
    models,
    weight_query,
    low_query,
    high_query,
    weight_key,
    low_key,
    high_key,
    weight_value,
    low_value,
    high_value,
    norm_train,
    norm_step,
):
    def spread(array):
        return [array] + [
            lax.ppermute(array, "shard", [((d + k) % shards, d) for d in range(shards)]) for k in range(1, shards)
        ]

    rank = low_query.shape[1]
    depth = -(-3 * rank // 128) * 128
    low = jnp.concatenate([low_query, low_key, low_value], axis=1)
    low = jnp.pad(low, ((0, 0), (0, depth - 3 * rank)))
    highs = [
        jnp.pad(mix_rate * high, ((k * rank, depth - (k + 1) * rank), (0, 0)))
        for k, high in enumerate((high_query, high_key, high_value))
    ]
    lows = spread(low)
    serve_norm = gather_norm(shards, models, (norm_train + norm_step).astype(jnp.bfloat16))
    final_query, factor_query = merge(shards, spread(weight_query), lows, highs[0])
    final_key, factor_key = merge(shards, spread(weight_key), lows, highs[1])
    final_value, factor_value = merge(shards, spread(weight_value), lows, highs[2])
    return (final_query, final_key, final_value, factor_query, factor_key, factor_value, serve_norm)


def solution(mesh):
    placed = (
        P(("copy", "shard"), "model"),
        P(("copy", "shard"), None),
        P("copy", "model"),
        P(("copy", "shard"), "model"),
        P(("copy", "shard"), None),
        P("copy", "model"),
        P(("copy", "shard"), "model"),
        P(("copy", "shard"), None),
        P("copy", "model"),
        P(("copy", "shard", "model")),
        P(("copy", "shard", "model")),
    )
    return jax.shard_map(
        functools.partial(on_device, mesh.shape["shard"], mesh.shape["model"]),
        mesh=mesh,
        in_specs=placed,
        out_specs=(
            P("copy", "model"),
            P("copy", "model"),
            P("copy", "model"),
            P(("copy", "model")),
            P(("copy", "model")),
            P(("copy", "model")),
            P("copy"),
        ),
        check_vma=False,
    )
```

```python
import functools

import jax
import jax.numpy as jnp
from jax import lax
from jax.experimental import pallas as pl
from jax.experimental.pallas import tpu as pltpu
from jax.sharding import PartitionSpec as P

mix_rate = 2.0
vmem_bytes = 67_000_000
MESH = pl.DeviceIdType.MESH


def chunk_of(rows):
    for chunk in (256, 128):
        if rows % chunk == 0:
            return chunk
    return rows


def steps_of(rows):
    for steps in (6, 3, 2):
        if rows % (steps * 128) == 0:
            return steps
    return 1


def width_of(columns):
    return 256 if columns % 256 == 0 else 128


def product(low, high):
    return lax.dot_general(low, high, (((0,), (0,)), ((), ())), preferred_element_type=jnp.float32)


def largest(result):
    rows, columns = result.shape
    return jnp.max(jnp.abs(result).reshape(rows // 8, 8, columns), axis=0)


def own_kernel(shards, models, steps, *refs):
    weights, lows, highs, norm_ref = refs[:3], refs[3:6], refs[6:9], refs[9]
    tops, norm_out = refs[10:13], refs[13]
    landed, send_sem, recv_sem = refs[14:]
    step = pl.program_id(0)
    shard, model = lax.axis_index("shard"), lax.axis_index("model")
    me = shard * models + model
    others = [
        (lax.rem(shard + s, shards), lax.rem(model + m, models), s * models + m)
        for s in range(shards)
        for m in range(models)
        if s or m
    ]

    def copies():
        return [
            pltpu.make_async_remote_copy(
                src_ref=norm_ref,
                dst_ref=landed.at[me],
                send_sem=send_sem.at[k],
                recv_sem=recv_sem.at[k],
                device_id={"shard": s, "model": m},
                device_id_type=MESH,
            )
            for s, m, k in others
        ]

    @pl.when(step == 0)
    def _():
        barrier = pltpu.get_barrier_semaphore()
        for s, m, _ in others:
            pl.semaphore_signal(barrier, inc=1, device_id={"shard": s, "model": m}, device_id_type=MESH)
        landed[me] = norm_ref[...]
        for top in tops:
            top[...] = jnp.zeros_like(top)

    @pl.when(step == min(2, steps - 1))
    def _():
        pl.semaphore_wait(pltpu.get_barrier_semaphore(), len(others))
        for copy in copies():
            copy.start()

    for weight, low, high, top in zip(weights, lows, highs, tops):
        rows, columns = weight.shape
        width = width_of(columns)
        for j in range(columns // width):
            at = pl.ds(j * width, width)
            result = weight[:, at].astype(jnp.float32) + product(low[...], high[:, at] * mix_rate)
            top[:, at] = jnp.maximum(top[:, at], largest(result))

    @pl.when(step == steps - 1)
    def _():
        for copy in copies():
            copy.wait()
        norm_out[...] = landed[...].reshape(norm_out.shape).astype(norm_out.dtype)


def own_part(shards, models, weights, lows, highs, norm):
    rows, rank = weights[0].shape[0], lows[0].shape[0]
    steps = steps_of(rows)
    part = rows // steps
    count, size = shards * models, norm.shape[0]
    whole = lambda shape: pl.BlockSpec(shape, lambda i: (0, 0))
    *tops, gathered = pl.pallas_call(
        functools.partial(own_kernel, shards, models, steps),
        grid=(steps,),
        out_shape=[jax.ShapeDtypeStruct((8, w.shape[1]), jnp.float32) for w in weights]
        + [jax.ShapeDtypeStruct((count, size), jnp.bfloat16)],
        in_specs=[pl.BlockSpec((part, w.shape[1]), lambda i: (i, 0)) for w in weights]
        + [pl.BlockSpec((rank, part), lambda i: (0, i))] * 3
        + [whole(h.shape) for h in highs]
        + [whole((1, size))],
        out_specs=[whole((8, w.shape[1])) for w in weights] + [whole((count, size))],
        scratch_shapes=[
            pltpu.VMEM((count, 1, size), jnp.float32),
            pltpu.SemaphoreType.DMA((count,)),
            pltpu.SemaphoreType.DMA((count,)),
        ],
        compiler_params=pltpu.CompilerParams(
            collective_id=0, has_side_effects=True, vmem_limit_bytes=vmem_bytes
        ),
        cost_estimate=pl.CostEstimate(
            flops=2 * rows * rank * sum(w.shape[1] for w in weights),
            bytes_accessed=2 * rows * sum(w.shape[1] for w in weights),
            transcendentals=0,
        ),
    )(*weights, *lows, *highs, norm.reshape(1, size))
    return tops, gathered.reshape(count * size)


def merge_kernel(n, *refs):
    parts, lows = refs[:n], refs[n : 2 * n]
    high_ref, top_ref, out_ref, factor_ref, held = refs[2 * n :]
    me = lax.axis_index("shard")
    rows, columns = parts[0].shape
    chunk = chunk_of(rows)
    high = high_ref[...] * mix_rate
    pieces = [pl.ds(i * chunk, chunk) for i in range(rows // chunk)]

    def result_of(k, at):
        return parts[k][at, :].astype(jnp.float32) + product(lows[k][:, at], high)

    top = top_ref[...]
    for k in range(1, n):
        for at in pieces:
            result = result_of(k, at)
            held[pl.ds((k - 1) * rows + at.start, chunk), :] = result
            top = jnp.maximum(top, largest(result))
    factor = jnp.max(top, axis=0, keepdims=True)
    factor_ref[...] = factor
    scale = 1.0 / factor
    for k in range(n):
        base = lax.rem(me + k, n) * rows
        for at in pieces:
            result = held[pl.ds((k - 1) * rows + at.start, chunk), :] if k else result_of(k, at)
            to = pl.ds(pl.multiple_of(base + at.start, 16), chunk)
            out_ref[to, :] = (result * scale).astype(out_ref.dtype)


def merge(n, parts, lows, high, top):
    rows, columns = parts[0].shape
    width = width_of(columns)
    rank = high.shape[0]
    final, factor = pl.pallas_call(
        functools.partial(merge_kernel, n),
        grid=(columns // width,),
        out_shape=(
            jax.ShapeDtypeStruct((n * rows, columns), jnp.bfloat16),
            jax.ShapeDtypeStruct((1, columns), jnp.float32),
        ),
        in_specs=[pl.BlockSpec((rows, width), lambda j: (0, j))] * n
        + [pl.BlockSpec((rank, rows), lambda j: (0, 0))] * n
        + [pl.BlockSpec((rank, width), lambda j: (0, j)), pl.BlockSpec((8, width), lambda j: (0, j))],
        out_specs=(
            pl.BlockSpec((n * rows, width), lambda j: (0, j)),
            pl.BlockSpec((1, width), lambda j: (0, j)),
        ),
        scratch_shapes=[pltpu.VMEM((max(n - 1, 1) * rows, width), jnp.float32)],
        compiler_params=pltpu.CompilerParams(vmem_limit_bytes=vmem_bytes),
        cost_estimate=pl.CostEstimate(
            flops=2 * n * rows * columns * rank, bytes_accessed=4 * n * rows * columns, transcendentals=0
        ),
    )(*parts, *lows, high, top)
    return final, factor.reshape(columns)


def on_device(
    shards,
    models,
    weight_query,
    low_query,
    high_query,
    weight_key,
    low_key,
    high_key,
    weight_value,
    low_value,
    high_value,
    norm_train,
    norm_step,
):
    def spread(array):
        return [array] + [
            lax.ppermute(array, "shard", [((d + k) % shards, d) for d in range(shards)]) for k in range(1, shards)
        ]

    weights = (weight_key, weight_value, weight_query)
    lows = [low.T for low in (low_key, low_value, low_query)]
    highs = (high_key, high_value, high_query)
    all_weights, all_lows = [], []
    for weight, low in zip(weights, lows):
        all_lows.append(spread(low))
        all_weights.append(spread(weight))
    tops, serve_norm = own_part(shards, models, weights, lows, highs, norm_train + norm_step)
    (final_key, factor_key), (final_value, factor_value), (final_query, factor_query) = [
        merge(shards, *each) for each in zip(all_weights, all_lows, highs, tops)
    ]
    return (final_query, final_key, final_value, factor_query, factor_key, factor_value, serve_norm)


def solution(mesh):
    placed = (
        P(("copy", "shard"), "model"),
        P(("copy", "shard"), None),
        P("copy", "model"),
        P(("copy", "shard"), "model"),
        P(("copy", "shard"), None),
        P("copy", "model"),
        P(("copy", "shard"), "model"),
        P(("copy", "shard"), None),
        P("copy", "model"),
        P(("copy", "shard", "model")),
        P(("copy", "shard", "model")),
    )
    return jax.shard_map(
        functools.partial(on_device, mesh.shape["shard"], mesh.shape["model"]),
        mesh=mesh,
        in_specs=placed,
        out_specs=(
            P("copy", "model"),
            P("copy", "model"),
            P("copy", "model"),
            P(("copy", "model")),
            P(("copy", "model")),
            P(("copy", "model")),
            P("copy"),
        ),
        check_vma=False,
    )
```

```python
import functools

import jax
import jax.numpy as jnp
from jax import lax
from jax.experimental import pallas as pl
from jax.experimental.pallas import tpu as pltpu
from jax.sharding import PartitionSpec as P

mix_rate = 2.0
vmem_bytes = 67_000_000
MESH = pl.DeviceIdType.MESH


def chunk_of(rows):
    for chunk in (256, 128):
        if rows % chunk == 0:
            return chunk
    return rows


def steps_of(rows):
    for steps in (6, 3, 2):
        if rows % (steps * 128) == 0:
            return steps
    return 1


def width_of(columns):
    return 256 if columns % 256 == 0 else 128


def product(low, high):
    return jnp.dot(low, high, preferred_element_type=jnp.float32)


def largest(result):
    rows, columns = result.shape
    return jnp.max(jnp.abs(result).reshape(rows // 8, 8, columns), axis=0)


def own_kernel(shards, models, steps, *refs):
    weights, lows, highs, norm_ref = refs[:3], refs[3:6], refs[6:9], refs[9]
    tops, norm_out = refs[10:13], refs[13]
    landed, send_sem, recv_sem = refs[14:]
    step = pl.program_id(0)
    shard, model = lax.axis_index("shard"), lax.axis_index("model")
    me = shard * models + model
    others = [
        (lax.rem(shard + s, shards), lax.rem(model + m, models), s * models + m)
        for s in range(shards)
        for m in range(models)
        if s or m
    ]

    def copies():
        return [
            pltpu.make_async_remote_copy(
                src_ref=norm_ref,
                dst_ref=landed.at[me],
                send_sem=send_sem.at[k],
                recv_sem=recv_sem.at[k],
                device_id={"shard": s, "model": m},
                device_id_type=MESH,
            )
            for s, m, k in others
        ]

    @pl.when(step == 0)
    def _():
        barrier = pltpu.get_barrier_semaphore()
        for s, m, _ in others:
            pl.semaphore_signal(barrier, inc=1, device_id={"shard": s, "model": m}, device_id_type=MESH)
        landed[me] = norm_ref[...]
        for top in tops:
            top[...] = jnp.zeros_like(top)

    @pl.when(step == min(2, steps - 1))
    def _():
        pl.semaphore_wait(pltpu.get_barrier_semaphore(), len(others))
        for copy in copies():
            copy.start()

    for weight, low, high, top in zip(weights, lows, highs, tops):
        rows, columns = weight.shape
        width = width_of(columns)
        turned = low[...].T
        for j in range(columns // width):
            at = pl.ds(j * width, width)
            result = weight[:, at].astype(jnp.float32) + product(turned, high[:, at] * mix_rate)
            top[:, at] = jnp.maximum(top[:, at], largest(result))

    @pl.when(step == steps - 1)
    def _():
        for copy in copies():
            copy.wait()
        norm_out[...] = landed[...].reshape(norm_out.shape).astype(norm_out.dtype)


def own_part(shards, models, weights, lows, highs, norm):
    rows, rank = weights[0].shape[0], lows[0].shape[0]
    steps = steps_of(rows)
    part = rows // steps
    count, size = shards * models, norm.shape[0]
    whole = lambda shape: pl.BlockSpec(shape, lambda i: (0, 0))
    *tops, gathered = pl.pallas_call(
        functools.partial(own_kernel, shards, models, steps),
        grid=(steps,),
        out_shape=[jax.ShapeDtypeStruct((8, w.shape[1]), jnp.float32) for w in weights]
        + [jax.ShapeDtypeStruct((count, size), jnp.bfloat16)],
        in_specs=[pl.BlockSpec((part, w.shape[1]), lambda i: (i, 0)) for w in weights]
        + [pl.BlockSpec((rank, part), lambda i: (0, i))] * 3
        + [whole(h.shape) for h in highs]
        + [whole((1, size))],
        out_specs=[whole((8, w.shape[1])) for w in weights] + [whole((count, size))],
        scratch_shapes=[
            pltpu.VMEM((count, 1, size), jnp.float32),
            pltpu.SemaphoreType.DMA((count,)),
            pltpu.SemaphoreType.DMA((count,)),
        ],
        compiler_params=pltpu.CompilerParams(
            collective_id=0, has_side_effects=True, vmem_limit_bytes=vmem_bytes
        ),
        cost_estimate=pl.CostEstimate(
            flops=2 * rows * rank * sum(w.shape[1] for w in weights),
            bytes_accessed=2 * rows * sum(w.shape[1] for w in weights),
            transcendentals=0,
        ),
    )(*weights, *lows, *highs, norm.reshape(1, size))
    return tops, gathered.reshape(count * size)


def merge_kernel(n, width, *refs):
    parts, refs = [refs[p * n : (p + 1) * n] for p in range(3)], refs[3 * n :]
    lows, refs = [refs[p * n : (p + 1) * n] for p in range(3)], refs[3 * n :]
    highs, tops, outs, factors = refs[:3], refs[3:6], refs[6:9], refs[9:12]
    fresh, staged, held, turned, in_sem, out_sem = refs[12:]
    me = lax.axis_index("shard")
    rows = fresh.shape[2]
    chunk = chunk_of(rows)
    pieces = [pl.ds(i * chunk, chunk) for i in range(rows // chunk)]
    counts = [part[0].shape[1] // width for part in parts]

    def columns_of(j):
        return pl.ds(pl.multiple_of(j * width, width), width)

    def fetch(p, j, slot):
        return [
            pltpu.make_async_copy(parts[p][k].at[:, columns_of(j)], fresh.at[slot, k], in_sem.at[slot, k])
            for k in range(n)
        ]

    def put(p, j, slot):
        return pltpu.make_async_copy(staged.at[slot], outs[p].at[:, columns_of(j)], out_sem.at[slot])

    def start(p, j, slot):
        for copy in fetch(p, j, slot):
            copy.start()

    start(0, 0, 0)
    for p in range(3):
        for k in range(n):
            turned[p, k] = lows[p][k][...].T
    done = 0
    for p in range(3):

        def body(j, carry, p=p, done=done):
            slot = lax.rem(j + done, 2)

            @pl.when(j + 1 < counts[p])
            def _():
                start(p, j + 1, 1 - slot)

            if p + 1 < 3:

                @pl.when(j + 1 == counts[p])
                def _():
                    start(p + 1, 0, 1 - slot)

            for copy in fetch(p, j, slot):
                copy.wait()
            columns = columns_of(j)
            high = highs[p][:, columns] * mix_rate

            def result_of(k, at):
                return fresh[slot, k, at, :].astype(jnp.float32) + product(turned[p, k, at, :], high)

            top = tops[p][:, columns]
            for k in range(1, n):
                for at in pieces:
                    result = result_of(k, at)
                    held[pl.ds((k - 1) * rows + at.start, chunk), :] = result
                    top = jnp.maximum(top, largest(result))
            factor = jnp.max(top, axis=0, keepdims=True)
            factors[p][:, columns] = factor
            scale = 1.0 / factor

            @pl.when(j + done >= 2)
            def _():
                put(p, j, slot).wait()

            for k in range(n):
                base = lax.rem(me + k, n) * rows
                for at in pieces:
                    result = held[pl.ds((k - 1) * rows + at.start, chunk), :] if k else result_of(k, at)
                    to = pl.ds(pl.multiple_of(base + at.start, 16), chunk)
                    staged[slot, to, :] = (result * scale).astype(staged.dtype)
            put(p, j, slot).start()
            return carry

        lax.fori_loop(0, counts[p], body, 0)
        done += counts[p]
    for step in range(max(done - 2, 0), done):
        put(2, 0, step % 2).wait()


def merge(n, parts, lows, highs, tops):
    rows = parts[0][0].shape[0]
    sizes = [part[0].shape[1] for part in parts]
    width = min(width_of(size) for size in sizes)
    rank = highs[0].shape[0]
    vmem, anywhere = pl.BlockSpec(memory_space=pltpu.VMEM), pl.BlockSpec(memory_space=pl.ANY)
    results = pl.pallas_call(
        functools.partial(merge_kernel, n, width),
        out_shape=[jax.ShapeDtypeStruct((n * rows, size), jnp.bfloat16) for size in sizes]
        + [jax.ShapeDtypeStruct((1, size), jnp.float32) for size in sizes],
        in_specs=[anywhere] * (3 * n) + [vmem] * (3 * n + 6),
        out_specs=[anywhere] * 3 + [vmem] * 3,
        scratch_shapes=[
            pltpu.VMEM((2, n, rows, width), jnp.bfloat16),
            pltpu.VMEM((2, n * rows, width), jnp.bfloat16),
            pltpu.VMEM((max(n - 1, 1) * rows, width), jnp.float32),
            pltpu.VMEM((3, n, rows, rank), jnp.bfloat16),
            pltpu.SemaphoreType.DMA((2, n)),
            pltpu.SemaphoreType.DMA((2,)),
        ],
        compiler_params=pltpu.CompilerParams(vmem_limit_bytes=vmem_bytes),
        cost_estimate=pl.CostEstimate(
            flops=2 * n * rows * sum(sizes) * rank, bytes_accessed=4 * n * rows * sum(sizes), transcendentals=0
        ),
    )(*[x for part in parts for x in part], *[x for low in lows for x in low], *highs, *tops)
    return results[:3], [factor.reshape(size) for factor, size in zip(results[3:], sizes)]


def on_device(
    shards,
    models,
    weight_query,
    low_query,
    high_query,
    weight_key,
    low_key,
    high_key,
    weight_value,
    low_value,
    high_value,
    norm_train,
    norm_step,
):
    def spread(array):
        return [array] + [
            lax.ppermute(array, "shard", [((d + k) % shards, d) for d in range(shards)]) for k in range(1, shards)
        ]

    weights = (weight_key, weight_value, weight_query)
    lows = [low.T for low in (low_key, low_value, low_query)]
    highs = (high_key, high_value, high_query)
    all_weights, all_lows = [], []
    for weight, low in zip(weights, lows):
        all_lows.append(spread(low))
        all_weights.append(spread(weight))
    tops, serve_norm = own_part(shards, models, weights, lows, highs, norm_train + norm_step)
    finals, factors = merge(shards, all_weights, all_lows, highs, tops)
    (final_key, final_value, final_query), (factor_key, factor_value, factor_query) = finals, factors
    return (final_query, final_key, final_value, factor_query, factor_key, factor_value, serve_norm)


def solution(mesh):
    placed = (
        P(("copy", "shard"), "model"),
        P(("copy", "shard"), None),
        P("copy", "model"),
        P(("copy", "shard"), "model"),
        P(("copy", "shard"), None),
        P("copy", "model"),
        P(("copy", "shard"), "model"),
        P(("copy", "shard"), None),
        P("copy", "model"),
        P(("copy", "shard", "model")),
        P(("copy", "shard", "model")),
    )
    return jax.shard_map(
        functools.partial(on_device, mesh.shape["shard"], mesh.shape["model"]),
        mesh=mesh,
        in_specs=placed,
        out_specs=(
            P("copy", "model"),
            P("copy", "model"),
            P("copy", "model"),
            P(("copy", "model")),
            P(("copy", "model")),
            P(("copy", "model")),
            P("copy"),
        ),
        check_vma=False,
    )
```
